32 devices in a mesh: bra: 8 (over z, x), ket: 2 (over y), mpo: 2 (over core).
Axes of the slice: x: 2, y: 2, z: 4, core: 2. Of those that a mesh axis runs over, the one named last changes fastest.
Arguments:
- left_env: bfloat16 [4, 3072, 3072], P('mpo', 'bra', 'ket'), may hold values from -6 to 6
- site_tensor: bfloat16 [3072, 4, 3072], P('bra', None, 'ket'), may hold values from -0.0546875 to 0.0546875
- block_values: float32 [12, 4, 4], replicated, may hold values from -3 to 3
- pair_in: int32 [12], replicated, may hold values from 0 to 3
- pair_out: int32 [12], replicated, may hold values from 0 to 3, as said below
Outputs:
- new_env: bfloat16 [4, 3072, 3072], P('mpo', 'bra', 'ket')
The draws below stay inside these ranges and needn't reach their ends.
Inputs may be any that keep to these rules, and one draw needn't show every extreme that they name: `pair_out`: every component number 0 to 3 appears at least once.
All inputs are finite; a program needn't handle non-finite values.
Results may differ from the reference program's by a relative error of at most 0.018.
Values may be sent and summed in bfloat16 or wider, within the bound.
A program may use at most 192 MiB of HBM per device.

```python
import jax
import jax.numpy as jnp
from jax import lax

D = 3072
PHYS = 4
K = 4
NNZ = 12
N_BRA = 8


def draw_pair_out(key, part):
    first = jax.random.permutation(jax.random.fold_in(key, 11), K).astype(jnp.int32)
    extra = jax.random.randint(jax.random.fold_in(key, 12), (NNZ - K,), 0, K).astype(jnp.int32)
    return jnp.concatenate([first, extra]).astype(jnp.int32)


def touch_ends(result, own_key, smallest, high):
    extent = result.shape
    spot = [jax.random.randint(jax.random.fold_in(own_key, axis), (), 0, extent[axis]) for axis in range(len(extent))]
    result = result.at[tuple(spot)].set(smallest)
    longest = extent.index(max(extent))
    spot[longest] = (spot[longest] + 1) % extent[longest]
    return result.at[tuple(spot)].set(high)


def steps_of(rng, dims, split, smallest, top_value):
    def one(dim, parts):
        steps = jax.random.uniform(jax.random.fold_in(jax.random.fold_in(rng, 6), dim), (parts,), jnp.float32, smallest / len(split), top_value / len(split))
        return jnp.repeat(jnp.exp(steps), dims[dim] // parts).reshape((-1,) + (1,) * (len(dims) - dim - 1))

    factor_of = one(*split[0])
    for cut in split[1:]:
        factor_of = factor_of * one(*cut)
    return factor_of


def bell_draw(rng, extent, width, bound, pieces=(), held_as=jnp.bfloat16):
    entries = width * jax.random.normal(rng, extent, jnp.float32)
    if pieces:
        entries = entries * steps_of(rng, extent, pieces, -0.22, 0.18)
    return jnp.clip(entries, -bound, bound).astype(held_as)


def setup_inputs(seed: int = 0) -> dict:
    streams_of = jax.random.split(jax.random.key(seed), 6)
    left_env = bell_draw(streams_of[0], (K, D, D), 1.0, 6.0, ((0, 2), (1, 8), (2, 2)))
    site_tensor = bell_draw(streams_of[1], (D, PHYS, D), (PHYS * D) ** -0.5, 0.0546875, ((0, 8), (2, 2)))
    block_values = bell_draw(streams_of[2], (NNZ, PHYS, PHYS), 0.5, 3.0, (), jnp.float32)
    pair_in = touch_ends(jax.random.randint(streams_of[3], (NNZ,), 0, K), jax.random.fold_in(streams_of[3], 1), 0, K - 1).astype(jnp.int32)
    pair_out = draw_pair_out(jax.random.fold_in(streams_of[5], 71), 0)
    return {"left_env": left_env, "site_tensor": site_tensor, "block_values": block_values, "pair_in": pair_in, "pair_out": pair_out}


def reference(left_env, site_tensor, block_values, pair_in, pair_out):
    comps = jnp.arange(K, dtype=jnp.int32)
    hot_out = (pair_out[:, None] == comps[None, :]).astype(jnp.float32)
    hot_in = (pair_in[:, None] == comps[None, :]).astype(jnp.float32)
    mixing = jnp.einsum("pv,pw,pst->vswt", hot_out, hot_in, block_values, precision=lax.Precision.HIGHEST)
    flat_site = site_tensor.reshape(D, PHYS * D)

    def one_comp(env):
        return jnp.dot(env, flat_site, preferred_element_type=jnp.float32).astype(jnp.bfloat16)

    half = lax.map(one_comp, left_env).reshape(K, D, PHYS, D)
    mixed = jnp.einsum("vswt,watc->vasc", mixing, half.astype(jnp.float32), precision=lax.Precision.HIGHEST).astype(jnp.bfloat16)
    rows_blk = D // N_BRA

    def add_block(index, total):
        start = (index * rows_blk).astype(jnp.int32)
        site_blk = lax.dynamic_slice_in_dim(site_tensor, start, rows_blk, 0).reshape(rows_blk * PHYS, D)
        mixed_blk = lax.dynamic_slice_in_dim(mixed, start, rows_blk, 1).reshape(K, rows_blk * PHYS, D)
        term = jnp.einsum("ke,wkc->wec", site_blk.astype(jnp.float32), mixed_blk.astype(jnp.float32))
        return total + term.astype(jnp.bfloat16).astype(jnp.float32)

    total = lax.fori_loop(0, N_BRA, add_block, jnp.zeros((K, D, D), jnp.float32))
    return total.astype(jnp.bfloat16)
```

```python
import jax
import jax.numpy as jnp
from jax import lax
from jax.sharding import PartitionSpec as P

K = 4


def local(left_env, site_tensor, block_values, pair_in, pair_out):
    comps_loc = left_env.shape[0]
    rows_loc = left_env.shape[1]
    cols_loc = left_env.shape[2]
    phys = site_tensor.shape[1]
    comps = jnp.arange(K, dtype=jnp.int32)
    hot_out = (pair_out[:, None] == comps[None, :]).astype(jnp.float32)
    hot_in = (pair_in[:, None] == comps[None, :]).astype(jnp.float32)
    mixing = jnp.einsum(
        "pv,pw,pst->vswt", hot_out, hot_in, block_values, precision=lax.Precision.HIGHEST
    )
    splits = lax.axis_size("mpo")
    half_cols = cols_loc // splits
    own_start = lax.axis_index("mpo") * half_cols
    site_own = lax.dynamic_slice_in_dim(site_tensor, own_start, half_cols, 2)
    site_full = lax.all_gather(
        site_own.reshape(rows_loc, phys * half_cols), "bra", axis=0, tiled=True
    )
    piece = lax.all_gather(left_env, "ket", axis=2, tiled=True)
    piece = lax.all_gather(piece, "mpo", axis=0, tiled=True)
    comps_all, width = piece.shape[0], piece.shape[2]
    half = jnp.dot(
        piece.reshape(comps_all * rows_loc, width), site_full, preferred_element_type=jnp.float32
    )
    half = half.astype(jnp.bfloat16).reshape(comps_all, rows_loc, phys, half_cols)
    mixed = jnp.einsum(
        "vswt,watc->savc", mixing, half.astype(jnp.float32), precision=lax.Precision.HIGHEST
    ).astype(jnp.bfloat16)
    mixed_pairs = mixed.reshape(phys * rows_loc, comps_all * half_cols)
    site_wide = lax.all_gather(
        jnp.transpose(site_tensor, (1, 0, 2)), "ket", axis=2, tiled=True
    )
    site_pairs = site_wide.reshape(phys * rows_loc, site_wide.shape[2])
    term = lax.dot_general(
        site_pairs, mixed_pairs, (((0,), (0,)), ((), ())), preferred_element_type=jnp.float32
    ).astype(jnp.bfloat16)
    owned = lax.psum_scatter(term, "bra", scatter_dimension=0, tiled=True)
    owned = jnp.transpose(owned.reshape(-1, comps_all, half_cols), (1, 0, 2))
    return lax.all_to_all(owned, "mpo", split_axis=0, concat_axis=2, tiled=True)


def solution(mesh):
    return jax.shard_map(
        local,
        mesh=mesh,
        in_specs=(P("mpo", "bra", "ket"), P("bra", None, "ket"), P(), P(), P()),
        out_specs=P("mpo", "bra", "ket"),
        check_vma=False,
    )
```
